256 devices in a mesh: freq: 8 (over x, z_lo), trial: 32 (over y, z_hi, core).
Axes of the slice: x: 4, y: 4, z: 8 (z_hi: 4, z_lo: 2; z = z_hi * 2 + z_lo), core: 2. Of those that a mesh axis runs over, the one named last changes fastest.
Arguments:
- signals: bfloat16 [64, 306, 1024], P('trial'), may hold values from -6 to 6
- kernel: bfloat16 [8192, 306], P('trial'), may hold values from -0.3125 to 0.3125
- freqs: float32 [40], P('freq'), may hold values from 3.6 to 66
Outputs:
- rel_power: float32 [8192, 640], P('trial', 'freq')
- itc_score: float32 [8192, 640], P('trial', 'freq')
The draws below stay inside these ranges and needn't reach their ends.
All inputs are finite; a program needn't handle non-finite values.
Results may differ from the reference program's by a relative error of at most 0.0003.
Values may be sent and summed in bfloat16 or wider, within the bound.
No kernel may reach another device: no remote copies, remote signals or barrier semaphores. Data moves between devices by JAX's collectives and lax.ppermute only.
A program may use at most 64 MiB of HBM per device.

```python
import jax
import jax.numpy as jnp
from jax import lax

C = 306
SRC = 8192
SAMPLES = 1024
TOUT = 16
FREQS = 40
TRIALS = 64


def draw_freqs(key, part):
    ladder = jnp.arange(FREQS, dtype=jnp.float32) / max(FREQS - 1, 1)
    base = 4.0 * jnp.exp(ladder * jnp.log(15.0))
    jitter = jax.random.uniform(key, (FREQS,), jnp.float32, 0.97, 1.03)
    values = base * jitter
    return jax.random.permutation(jax.random.fold_in(key, 7), values).astype(jnp.float32)


def level_of(stream_key, dims, shards, low, top_value):
    def one(axis_at, shards_of):
        draws = jax.random.uniform(jax.random.fold_in(jax.random.fold_in(stream_key, 6), axis_at), (shards_of,), jnp.float32, low / len(shards), top_value / len(shards))
        return jnp.repeat(jnp.exp(draws), dims[axis_at] // shards_of).reshape((-1,) + (1,) * (len(dims) - axis_at - 1))

    level = one(*shards[0])
    for cut in shards[1:]:
        level = level * one(*cut)
    return level


def gaussian(stream_key, shape, width, bound, cuts=(), kind=jnp.bfloat16):
    array = width * jax.random.normal(stream_key, shape, jnp.float32)
    if cuts:
        array = array * level_of(stream_key, shape, cuts, -0.22, 0.18)
    return jnp.clip(array, -bound, bound).astype(kind)


def setup_inputs(seed: int = 0) -> dict:
    streams_of = jax.random.split(jax.random.key(seed), 4)
    return {
        "signals": gaussian(streams_of[0], (TRIALS, C, SAMPLES), 1.0, 6.0, ((0, 32),)),
        "kernel": gaussian(streams_of[1], (SRC, C), C ** -0.5, 0.3125, ((0, 32),)),
        "freqs": draw_freqs(jax.random.fold_in(streams_of[3], 71), 0),
    }


CYCLES = 7.0
SAMPLE_RATE = 1000.0
PHASE_FLOOR = 0.25
MEAN_EPSILON = 1e-06

def wavelet_table(frequencies, sample_count, point_count):
    stride = sample_count // point_count
    moments = jnp.arange(sample_count, dtype=frequencies.dtype)[:, None, None]
    centres = (jnp.arange(point_count, dtype=frequencies.dtype) * stride + stride // 2)[None, None, :]
    widths = CYCLES * SAMPLE_RATE / (2.0 * jnp.pi) / frequencies[None, :, None]
    offset = moments - centres
    envelope = jnp.exp(-offset * offset / (2.0 * widths * widths)) * (8.0 / widths)
    angles = 2.0 * jnp.pi / SAMPLE_RATE * frequencies[None, :, None] * offset
    stacked = jnp.stack([envelope * jnp.cos(angles), envelope * jnp.sin(angles)], axis=1)
    return stacked.reshape(sample_count, -1)

def reference(signals, kernel, freqs):
    trial_count, chan_count, sample_count = signals.shape
    table = wavelet_table(freqs, sample_count, TOUT)
    flat = signals.reshape(trial_count * chan_count, sample_count).astype(jnp.float32)
    coefficients = jnp.dot(flat, table, precision=lax.Precision.HIGHEST, preferred_element_type=jnp.float32)
    coefficients = coefficients.reshape(trial_count, chan_count, -1)
    span = FREQS * TOUT
    kernel_wide = kernel.astype(jnp.float32)

    def one_trial(carry, block):
        source = jnp.dot(kernel_wide, block, precision=lax.Precision.HIGHEST)
        real_part = source[:, :span]
        imag_part = source[:, span:]
        magnitude = real_part * real_part + imag_part * imag_part
        inverse = lax.rsqrt(magnitude + PHASE_FLOOR)
        return ((carry[0] + magnitude, carry[1] + real_part * inverse, carry[2] + imag_part * inverse), None)
    zeros_init = jnp.zeros((SRC, span), jnp.float32)
    sums, unused = lax.scan(one_trial, (zeros_init, zeros_init, zeros_init), coefficients)
    power = sums[0] / TRIALS
    mean_power = lax.optimization_barrier(jnp.sum(power, axis=1, keepdims=True)) / (FREQS * TOUT)
    rel_power = power / (mean_power + MEAN_EPSILON)
    itc_score = (sums[1] * sums[1] + sums[2] * sums[2]) / TRIALS
    return (rel_power, itc_score)
```

```python
import jax
import jax.numpy as jnp
from jax import lax
from jax.experimental import pallas as pl
from jax.experimental.pallas import tpu as pltpu
from jax.sharding import PartitionSpec as P

TOUT = 16
CYCLES = 7.0
SAMPLE_RATE = 1000.0
PHASE_FLOOR = 0.25
MEAN_EPSILON = 1e-06

LEVELS = 30000.0
STEPS = 128.0
CENTRE = 120.0

BOTH = ("freq", "trial")


def place_of(index):
    freq, trial = divmod(index, 32)
    return freq // 2, freq % 2, trial // 8, trial // 2 % 4, trial % 2


def index_of(x, z_lo, y, z_hi, core):
    return (x * 2 + z_lo) * 32 + y * 8 + z_hi * 2 + core


def moved(value, rule):
    count = lax.axis_size("freq") * lax.axis_size("trial")
    return lax.ppermute(value, BOTH, [(i, index_of(*rule(*place_of(i)))) for i in range(count)])


def along_y(step):
    return lambda x, zl, y, zh, c: (x, zl, (y + step) % 4, zh, c)


def other_core(x, zl, y, zh, c):
    return x, zl, y, zh, 1 - c


def next_pair(x, zl, y, zh, c):
    return x, 1 - zl, y, (zh + (1 if zl else -1)) % 4, c


def same_pair(x, zl, y, zh, c):
    return x, 1 - zl, y, zh, c


def near(x, zl, y, zh, c):
    return x, zl, y, (zh + (1 if zl else -1)) % 4, c


def far(x, zl, y, zh, c):
    return x, zl, y, (zh + (-1 if zl else 1)) % 4, c


def opposite(x, zl, y, zh, c):
    return x, zl, y, (zh + 2) % 4, c


def encoded(level):
    size = jnp.abs(level)
    octave = jnp.floor(size * (1.0 / STEPS))
    value = (1.0 + (size - octave * STEPS) * (1.0 / STEPS)) * jnp.exp2(octave - CENTRE)
    return jnp.where(level < 0.0, -value, value).astype(jnp.bfloat16)


def decoded(code):
    value = code.astype(jnp.float32)
    size = jnp.abs(value)
    octave = jnp.floor(jnp.log2(size))
    level = STEPS * (octave + (CENTRE - 1.0)) + STEPS * size * jnp.exp2(-octave)
    return jnp.where(value < 0.0, -level, level)


def split(value):
    high = value.astype(jnp.bfloat16)
    return high, (value - high.astype(jnp.float32)).astype(jnp.bfloat16)


def nt(a, b):
    return lax.dot_general(a, b, (((1,), (1,)), ((), ())), preferred_element_type=jnp.float32)


def lanes_of(shape):
    return lax.broadcasted_iota(jnp.int32, shape, 1)


def coefficients_body(signals, waves, wire, shifts, table, rest):
    samples = signals.shape[2]
    span = table.shape[0] // 4
    tail = signals.shape[1] - 256
    length = waves.shape[1]
    stride = samples // TOUT
    waves = waves[...]
    turned = pltpu.roll(waves, length - stride, 1)
    for point in range(TOUT):
        start = samples - stride * (point + 1)
        part = waves if start % 128 == 0 else turned
        start -= start % 128
        for cut in range(0, samples, 128):
            piece = part[:, start + cut : start + cut + 128]
            first = cut // 128 * 2 * span + point
            shifts[pl.ds(first, waves.shape[0], stride=TOUT), :] = piece
    for cut in range(0, samples, 128):
        first = cut // 128 * 2 * span
        high, low = split(shifts[first : first + 2 * span, :])
        table[: 2 * span, cut : cut + 128] = high
        table[2 * span :, cut : cut + 128] = low
    rest[...] = jnp.zeros(rest.shape, rest.dtype)
    rest[:tail, :] = signals[0, 256:, :]
    rest[64 : 64 + tail, :] = signals[1, 256:, :]
    both = nt(table[...], rest[...])
    ends = both[: 2 * span] + both[2 * span :]
    lane = lanes_of(ends.shape)
    first = lane < 64
    used = (lane & 63) < tail
    sizes = jnp.where(used, jnp.abs(ends), 0.0)
    scales = []
    for n in range(2):
        both = nt(table[...], signals[n, :256, :])
        main = both[: 2 * span] + both[2 * span :]
        own = jnp.where(first == (n == 0), sizes, 0.0)
        top = jnp.maximum(jnp.maximum(jnp.abs(main[:, :128]), jnp.abs(main[:, 128:])), own)
        top = jnp.max(top, axis=1, keepdims=True) * 1.01 + 1e-30
        top = top.astype(jnp.bfloat16).astype(jnp.float32)
        level = encoded(jnp.round(main * (LEVELS / top)))
        wire[n * 2 * span : (n + 1) * 2 * span, :] = level[:, :128]
        wire[(n + 2) * 2 * span : (n + 3) * 2 * span, :] = level[:, 128:]
        scales.append(top)
    scale = jnp.where(first, scales[0], scales[1])
    level = encoded(jnp.round(jnp.where(used, ends, 0.0) * (LEVELS / scale)))
    level = jnp.where((lane & 63) == tail, scale, level.astype(jnp.float32))
    wire[8 * span : 10 * span, :] = level.astype(jnp.bfloat16)


def columns_body(tail, *refs):
    wires, out = refs[:-1], refs[-1]
    for at, wire in enumerate(wires):
        span = wire.shape[0] // 10
        ends = wire[8 * span : 10 * span, :]
        raw = ends.astype(jnp.float32)
        ends = decoded(ends)
        first = lanes_of(ends.shape) < 64
        for n in range(2):
            scale = raw[:, 64 * n + tail : 64 * n + tail + 1] * (1.0 / LEVELS)
            base = (at * 2 + n) * 2 * span
            rows = slice(base, base + 2 * span)
            for half in range(2):
                start = (half * 2 + n) * 2 * span
                high, low = split(decoded(wire[start : start + 2 * span, :]) * scale)
                out[rows, half * 128 : half * 128 + 128] = high
                out[rows, 256 + half * 128 : 384 + half * 128] = low
            values = ends * scale
            if n == 1:
                values = pltpu.roll(values, 64, 1)
            high = values.astype(jnp.bfloat16).astype(jnp.float32)
            low = pltpu.roll(values - high, 64, 1)
            out[rows, 512:640] = jnp.where(first, high, low).astype(jnp.bfloat16)


def partials_body(send, *refs):
    groups, kernel, out, weights, sums = refs[:-4], refs[-4], refs[-3], refs[-2], refs[-1]
    tail = kernel.shape[0] - 256
    weights[0:256, :] = kernel[0:256, :]
    weights[256:512, :] = kernel[0:256, :]
    weights[512:640, :] = jnp.zeros((128, weights.shape[1]), weights.dtype)
    weights[512 : 512 + tail, :] = kernel[256:, :]
    weights[576 : 576 + tail, :] = kernel[256:, :]
    span = sums.shape[0] // 3
    sums[...] = jnp.zeros(sums.shape, sums.dtype)
    trials = sum(group.shape[0] for group in groups) // (2 * span)
    for group in groups:

        def step(i, carry):
            block = group[pl.ds(i * 4 * span, 4 * span), :]
            source = jnp.dot(block, weights[...], preferred_element_type=jnp.float32)
            for n in range(2):
                real = source[n * 2 * span : n * 2 * span + span]
                imag = source[n * 2 * span + span : (n + 1) * 2 * span]
                size = real * real + imag * imag
                inverse = lax.rsqrt(size + PHASE_FLOOR)
                sums[0:span, :] += size
                sums[span : 2 * span, :] += real * inverse
                sums[2 * span : 3 * span, :] += imag * inverse
            return carry

        lax.fori_loop(0, group.shape[0] // (4 * span), step, 0)
    if not send:
        out[...] = sums[...]
        return
    power = sums[0:span, :]
    top = jnp.max(power, axis=0, keepdims=True) * 1.01 + 1e-30
    top = top.astype(jnp.bfloat16)
    scale = (2.0 * LEVELS) / top.astype(jnp.float32)
    out[0:span, :] = encoded(jnp.round(power * scale - LEVELS))
    out[span : 3 * span, :] = encoded(jnp.round(sums[span : 3 * span, :] * (LEVELS / trials)))
    out[3 * span : 3 * span + 16, :] = jnp.broadcast_to(top, (16, top.shape[1]))


def totals_body(trials, all_trials, own, *refs):
    wires, power, score, sums = refs[:-3], refs[-3], refs[-2], refs[-1]
    span = power.shape[0]
    total = own[0:span, :]
    phases = own[span : 3 * span, :]
    for wire in wires:
        top = wire[3 * span : 3 * span + 16, :].astype(jnp.float32)[0:1]
        total += (decoded(wire[0:span, :]) + LEVELS) * (top * (0.5 / LEVELS))
        phases += decoded(wire[span : 3 * span, :]) * (trials / LEVELS)
    total = total * (1.0 / all_trials)
    power[...] = total
    real, imag = phases[:span], phases[span:]
    score[...] = (real * real + imag * imag) * (1.0 / all_trials)
    sums[...] = jnp.sum(total, axis=0, keepdims=True)


def scaled_body(columns, power, sums, out):
    mean = jnp.sum(sums[...], axis=0) / columns
    out[...] = power[...] / (mean + MEAN_EPSILON)


def waves_of(frequencies, sample_count):
    stride = sample_count // TOUT
    offset = jnp.arange(2 * sample_count, dtype=jnp.float32)[None, :] - (sample_count - stride // 2)
    widths = CYCLES * SAMPLE_RATE / (2.0 * jnp.pi) / frequencies[:, None]
    envelope = jnp.exp(-offset * offset / (2.0 * widths * widths)) * (8.0 / widths)
    angles = 2.0 * jnp.pi / SAMPLE_RATE * frequencies[:, None] * offset
    return jnp.concatenate([envelope * jnp.cos(angles), envelope * jnp.sin(angles)], axis=0)


def call(body, shape, dtype, *args, scratch=(), name=None):
    many = isinstance(dtype, (list, tuple))
    shapes = (
        [jax.ShapeDtypeStruct(s, d) for s, d in zip(shape, dtype)]
        if many
        else jax.ShapeDtypeStruct(shape, dtype)
    )
    return pl.pallas_call(
        body,
        out_shape=shapes,
        scratch_shapes=list(scratch),
        name=name,
    )(*args)


def shards(signals, kernel, freqs):
    trial_count, chan_count, sample_count = signals.shape
    span = freqs.shape[0] * TOUT
    rows = kernel.shape[0]
    tail = chan_count - 256
    all_trials = trial_count * lax.axis_size("trial")
    bf16, f32 = jnp.bfloat16, jnp.float32

    kernel_own = kernel.T
    kernel_near = moved(kernel_own, next_pair)
    kernel_far = moved(kernel_near, same_pair)
    kernel_opposite = moved(kernel_far, next_pair)

    wire = call(
        coefficients_body,
        (10 * span, 128),
        bf16,
        signals,
        waves_of(freqs, sample_count),
        scratch=[
            pltpu.VMEM((sample_count // 128 * 2 * span, 128), f32),
            pltpu.VMEM((4 * span, sample_count), bf16),
            pltpu.VMEM((128, sample_count), bf16),
        ],
        name="coefficients",
    )
    others = [moved(wire, along_y(step)) for step in (2, 1, -1)]
    twin = moved(wire, other_core)
    twins = [moved(other, other_core) for other in others]

    def columns(*wires):
        return call(
            lambda *refs: columns_body(tail, *refs),
            (len(wires) * 4 * span, 640),
            bf16,
            *wires,
            name="columns",
        )

    groups = [columns(wire, twin), columns(*others, *twins)]

    def partials(rows_of, send):
        return call(
            lambda *refs: partials_body(send, *refs),
            (3 * span + 16, rows) if send else (3 * span, rows),
            bf16 if send else f32,
            *groups,
            rows_of,
            scratch=[pltpu.VMEM((640, rows), bf16), pltpu.VMEM((3 * span, rows), f32)],
            name="partials",
        )

    received = [
        moved(partials(kernel_opposite, True), opposite),
        moved(partials(kernel_near, True), near),
        moved(partials(kernel_far, True), far),
    ]
    own = partials(kernel_own, False)
    trials = 8 * trial_count
    power, score, sums = call(
        lambda *refs: totals_body(trials, all_trials, *refs),
        [(span, rows), (span, rows), (1, rows)],
        [f32, f32, f32],
        own,
        *received,
        name="totals",
    )
    count = lax.axis_size("freq")
    copies = jnp.broadcast_to(sums[None], (count, 1, rows))
    sums = lax.all_to_all(copies, "freq", 0, 0, tiled=True)
    columns_in_all = float(span * count)
    rel_power = call(
        lambda *refs: scaled_body(columns_in_all, *refs),
        (span, rows),
        f32,
        power,
        sums,
        name="scaled",
    )
    return rel_power.T, score.T


def solution(mesh):
    placed = (P("trial", None, None), P("trial", None), P("freq"))
    return jax.shard_map(
        shards,
        mesh=mesh,
        in_specs=placed,
        out_specs=(P("trial", "freq"), P("trial", "freq")),
        check_vma=False,
    )
```

```python
import jax
import jax.numpy as jnp
from jax import lax
from jax.experimental import pallas as pl
from jax.experimental.pallas import tpu as pltpu
from jax.sharding import PartitionSpec as P

TOUT = 16
CYCLES = 7.0
SAMPLE_RATE = 1000.0
PHASE_FLOOR = 0.25
MEAN_EPSILON = 1e-06

LEVELS = 30000.0
STEPS = 128.0
CENTRE = 120.0

BOTH = ("freq", "trial")


def place_of(index):
    freq, trial = divmod(index, 32)
    return freq // 2, freq % 2, trial // 8, trial // 2 % 4, trial % 2


def index_of(x, z_lo, y, z_hi, core):
    return (x * 2 + z_lo) * 32 + y * 8 + z_hi * 2 + core


def moved(value, rule):
    count = lax.axis_size("freq") * lax.axis_size("trial")
    return lax.ppermute(value, BOTH, [(i, index_of(*rule(*place_of(i)))) for i in range(count)])


def along_y(step):
    return lambda x, zl, y, zh, c: (x, zl, (y + step) % 4, zh, c)


def other_core(x, zl, y, zh, c):
    return x, zl, y, zh, 1 - c


def next_pair(x, zl, y, zh, c):
    return x, 1 - zl, y, (zh + (1 if zl else -1)) % 4, c


def same_pair(x, zl, y, zh, c):
    return x, 1 - zl, y, zh, c


def near(x, zl, y, zh, c):
    return x, zl, y, (zh + (1 if zl else -1)) % 4, c


def far(x, zl, y, zh, c):
    return x, zl, y, (zh + (-1 if zl else 1)) % 4, c


def opposite(x, zl, y, zh, c):
    return x, zl, y, (zh + 2) % 4, c


def encoded(level):
    size = jnp.abs(level)
    octave = jnp.floor(size * (1.0 / STEPS))
    value = (1.0 + (size - octave * STEPS) * (1.0 / STEPS)) * jnp.exp2(octave - CENTRE)
    return jnp.where(level < 0.0, -value, value).astype(jnp.bfloat16)


def decoded(code):
    value = code.astype(jnp.float32)
    size = jnp.abs(value)
    octave = jnp.floor(jnp.log2(size))
    level = STEPS * (octave + (CENTRE - 1.0)) + STEPS * size * jnp.exp2(-octave)
    return jnp.where(value < 0.0, -level, level)


def split(value):
    high = value.astype(jnp.bfloat16)
    return high, (value - high.astype(jnp.float32)).astype(jnp.bfloat16)


def nt(a, b):
    return lax.dot_general(a, b, (((1,), (1,)), ((), ())), preferred_element_type=jnp.float32)


def lanes_of(shape):
    return lax.broadcasted_iota(jnp.int32, shape, 1)


def coefficients_body(signals, waves, wire, shifts, table, sides):
    samples = signals.shape[2]
    span = table.shape[0] // 4
    tail = signals.shape[0] - 256
    side = sides.shape[0] // 2
    length = waves.shape[1]
    stride = samples // TOUT
    waves = waves[...]
    turned = pltpu.roll(waves, length - stride, 1)
    for point in range(TOUT):
        start = samples - stride * (point + 1)
        part = waves if start % 128 == 0 else turned
        start -= start % 128
        for cut in range(0, samples, 128):
            piece = part[:, start + cut : start + cut + 128]
            first = cut // 128 * 2 * span + point
            shifts[pl.ds(first, waves.shape[0], stride=TOUT), :] = piece
    for cut in range(0, samples, 128):
        first = cut // 128 * 2 * span
        high, low = split(shifts[first : first + 2 * span, :])
        table[: 2 * span, cut : cut + 128] = high
        table[2 * span :, cut : cut + 128] = low
    chans = signals.shape[0]
    merged = signals[...].reshape(2 * chans, samples)
    for at, columns in enumerate((slice(0, 128), slice(128, 2 * span))):
        lows = slice(2 * span + columns.start, 2 * span + columns.stop)
        found = nt(merged, table[columns, :]) + nt(merged, table[lows, :])
        sides[at * side : at * side + 2 * chans, : columns.stop - columns.start] = found
    lane = lanes_of((2 * span, 128))
    first = lane < 64
    used = lane < tail
    scales, ends = [], []
    for n in range(2):
        parts = []
        for at in range(2):
            part = sides[pl.ds(at * side + n, side // 2, stride=2), :]
            parts.append(part.T[: min(2 * span - 128 * at, 128), :])
        values = jnp.concatenate(parts, axis=0)
        main = values[:, :256]
        end = jnp.where(used, values[:, 256:384], 0.0)
        top = jnp.maximum(jnp.maximum(jnp.abs(main[:, :128]), jnp.abs(main[:, 128:])), jnp.abs(end))
        top = jnp.max(top, axis=1, keepdims=True) * 1.01 + 1e-30
        top = top.astype(jnp.bfloat16).astype(jnp.float32)
        level = encoded(jnp.round(main * (LEVELS / top)))
        wire[n * 2 * span : (n + 1) * 2 * span, :] = level[:, :128]
        wire[(n + 2) * 2 * span : (n + 3) * 2 * span, :] = level[:, 128:]
        scales.append(top)
        ends.append(jnp.round(end * (LEVELS / top)))
    level = encoded(jnp.where(first, ends[0], pltpu.roll(ends[1], 64, 1)))
    scale = jnp.where(first, scales[0], scales[1])
    level = jnp.where((lane & 63) == tail, scale, level.astype(jnp.float32))
    wire[8 * span : 10 * span, :] = level.astype(jnp.bfloat16)


def columns_body(tail, *refs):
    wires, out = refs[:-1], refs[-1]
    for at, wire in enumerate(wires):
        span = wire.shape[0] // 10
        ends = wire[8 * span : 10 * span, :]
        raw = ends.astype(jnp.float32)
        ends = decoded(ends)
        first = lanes_of(ends.shape) < 64
        for n in range(2):
            scale = raw[:, 64 * n + tail : 64 * n + tail + 1] * (1.0 / LEVELS)
            base = (at * 2 + n) * 2 * span
            rows = slice(base, base + 2 * span)
            for half in range(2):
                start = (half * 2 + n) * 2 * span
                high, low = split(decoded(wire[start : start + 2 * span, :]) * scale)
                out[rows, half * 128 : half * 128 + 128] = high
                out[rows, 256 + half * 128 : 384 + half * 128] = low
            values = ends * scale
            if n == 1:
                values = pltpu.roll(values, 64, 1)
            high = values.astype(jnp.bfloat16).astype(jnp.float32)
            low = pltpu.roll(values - high, 64, 1)
            out[rows, 512:640] = jnp.where(first, high, low).astype(jnp.bfloat16)


def partials_body(send, *refs):
    groups, kernel, out, weights, sources = refs[:-4], refs[-4], refs[-3], refs[-2], refs[-1]
    tail = kernel.shape[0] - 256
    weights[0:256, :] = kernel[0:256, :]
    weights[256:512, :] = kernel[0:256, :]
    weights[512:640, :] = jnp.zeros((128, weights.shape[1]), weights.dtype)
    weights[512 : 512 + tail, :] = kernel[256:, :]
    weights[576 : 576 + tail, :] = kernel[256:, :]
    at = 0
    for group in groups:
        count = group.shape[0]
        sources[at : at + count, :] = jnp.dot(
            group[...], weights[...], preferred_element_type=jnp.float32
        )
        at += count
    span = groups[0].shape[0] // 4
    trials = at // (2 * span)
    powers = []
    for start in range(0, span, 8):
        power = phase_real = phase_imag = 0.0
        for n in range(trials):
            real = sources[n * 2 * span + start : n * 2 * span + start + 8, :]
            imag = sources[n * 2 * span + span + start : n * 2 * span + span + start + 8, :]
            size = real * real + imag * imag
            inverse = lax.rsqrt(size + PHASE_FLOOR)
            power += size
            phase_real += real * inverse
            phase_imag += imag * inverse
        for part, sums in enumerate((power, phase_real, phase_imag)):
            if send and part == 0:
                powers.append(sums)
                continue
            if send:
                sums = jnp.round(sums * (LEVELS / trials))
            rows = slice(part * span + start, part * span + start + 8)
            out[rows, :] = encoded(sums) if send else sums
    if not send:
        return
    power = jnp.concatenate(powers, axis=0)
    top = jnp.max(power, axis=0, keepdims=True) * 1.01 + 1e-30
    top = top.astype(jnp.bfloat16)
    scale = (2.0 * LEVELS) / top.astype(jnp.float32)
    out[0:span, :] = encoded(jnp.round(power * scale - LEVELS))
    out[3 * span : 3 * span + 16, :] = jnp.broadcast_to(top, (16, top.shape[1]))


def totals_body(trials, all_trials, own, *refs):
    wires, power, score, sums = refs[:-3], refs[-3], refs[-2], refs[-1]
    span = power.shape[0]
    total = own[0:span, :]
    phases = own[span : 3 * span, :]
    for wire in wires:
        top = wire[3 * span : 3 * span + 16, :].astype(jnp.float32)[0:1]
        total += (decoded(wire[0:span, :]) + LEVELS) * (top * (0.5 / LEVELS))
        phases += decoded(wire[span : 3 * span, :]) * (trials / LEVELS)
    total = total * (1.0 / all_trials)
    power[...] = total
    real, imag = phases[:span], phases[span:]
    score[...] = (real * real + imag * imag) * (1.0 / all_trials)
    sums[...] = jnp.broadcast_to(jnp.sum(total, axis=0, keepdims=True)[None], sums.shape)


def scaled_body(columns, power, sums, out):
    mean = jnp.sum(sums[...], axis=0) / columns
    out[...] = power[...] / (mean + MEAN_EPSILON)


def waves_of(frequencies, sample_count):
    stride = sample_count // TOUT
    offset = jnp.arange(2 * sample_count, dtype=jnp.float32)[None, :] - (sample_count - stride // 2)
    widths = CYCLES * SAMPLE_RATE / (2.0 * jnp.pi) / frequencies[:, None]
    envelope = jnp.exp(-offset * offset / (2.0 * widths * widths)) * (8.0 / widths)
    angles = 2.0 * jnp.pi / SAMPLE_RATE * frequencies[:, None] * offset
    return jnp.concatenate([envelope * jnp.cos(angles), envelope * jnp.sin(angles)], axis=0)


def call(body, outs, *args, scratch=(), name=None, final=()):
    shapes = [
        jax.ShapeDtypeStruct(*out) if at in final else pltpu.VMEM(*out)
        for at, out in enumerate(outs)
    ]
    found = pl.pallas_call(
        body,
        out_shape=shapes,
        scratch_shapes=list(scratch),
        compiler_params=pltpu.CompilerParams(vmem_limit_bytes=24 * 2**20),
        name=name,
    )(*args)
    return found if len(outs) > 1 else found[0]


def shards(signals, kernel, freqs):
    trial_count, chan_count, sample_count = signals.shape
    span = freqs.shape[0] * TOUT
    rows = kernel.shape[0]
    tail = chan_count - 256
    all_trials = trial_count * lax.axis_size("trial")
    bf16, f32 = jnp.bfloat16, jnp.float32

    kernel_own = kernel.T
    kernel_near = moved(kernel_own, next_pair)
    kernel_far = moved(kernel_near, same_pair)
    kernel_opposite = moved(kernel_far, next_pair)

    wire = call(
        coefficients_body,
        [((10 * span, 128), bf16)],
        jnp.transpose(signals, (1, 0, 2)),
        waves_of(freqs, sample_count),
        scratch=[
            pltpu.VMEM((sample_count // 128 * 2 * span, 128), f32),
            pltpu.VMEM((4 * span, sample_count), bf16),
            pltpu.VMEM((2 * 768, 128), f32),
        ],
        name="coefficients",
    )
    others = [moved(wire, along_y(step)) for step in (2, 1, -1)]
    twin = moved(wire, other_core)
    twins = [moved(other, other_core) for other in others]

    def columns(*wires):
        return call(
            lambda *refs: columns_body(tail, *refs),
            [((len(wires) * 4 * span, 640), bf16)],
            *wires,
            name="columns",
        )

    groups = [columns(value) for value in (wire, twin, *others, *twins)]

    def partials(rows_of, send):
        return call(
            lambda *refs: partials_body(send, *refs),
            [((3 * span + 16, rows), bf16) if send else ((3 * span, rows), f32)],
            *groups,
            rows_of,
            scratch=[pltpu.VMEM((640, rows), bf16), pltpu.VMEM((32 * span, rows), f32)],
            name="partials",
        )

    received = [
        moved(partials(kernel_opposite, True), opposite),
        moved(partials(kernel_near, True), near),
        moved(partials(kernel_far, True), far),
    ]
    own = partials(kernel_own, False)
    trials = 8 * trial_count
    count = lax.axis_size("freq")
    power, score, sums = call(
        lambda *refs: totals_body(trials, all_trials, *refs),
        [((span, rows), f32), ((span, rows), f32), ((count, 1, rows), f32)],
        own,
        *received,
        name="totals",
        final=(1,),
    )
    sums = lax.all_to_all(sums, "freq", 0, 0, tiled=True)
    columns_in_all = float(span * count)
    rel_power = call(
        lambda *refs: scaled_body(columns_in_all, *refs),
        [((span, rows), f32)],
        power,
        sums,
        name="scaled",
        final=(0,),
    )
    return rel_power.T, score.T


def solution(mesh):
    placed = (P("trial", None, None), P("trial", None), P("freq"))
    return jax.shard_map(
        shards,
        mesh=mesh,
        in_specs=placed,
        out_specs=(P("trial", "freq"), P("trial", "freq")),
        check_vma=False,
    )
```
